8 devices in a mesh: data: 2 (over z, y), tp: 4 (over x, core).
Axes of the slice: x: 2, y: 2, z: 1, core: 2. Of those that a mesh axis runs over, the one named last changes fastest.
Arguments:
- attn_ctx: bfloat16 [4096, 8192], P('data', 'tp'), parts along dimension 0
- w_attn_out: bfloat16 [8192, 8192], P('tp')
- mlp_act: bfloat16 [4096, 32768], P('data', 'tp'), parts along dimension 0
- w_mlp_down: bfloat16 [32768, 8192], P('tp')
Outputs:
- output: bfloat16 [4096, 8192], P('data'), parts along dimension 0
There are 2 independent parts. The reference program is written for one: setup_inputs(seed, part) draws one part's arguments, and reference() takes and returns one part's arrays. A program takes and returns all parts, laid end to end along the dimension named above; an argument that names none is the same for every part.
All inputs are finite; a program needn't handle non-finite values.
Results may differ from the reference program's by a relative error of at most 0.0102996.
Values are sent between devices in bfloat16 or wider.
A program may use at most 1 GiB of HBM per device.

```python
import jax
import jax.numpy as jnp

TOKENS = 2048
HIDDEN = 8192
FFN_DIM = 32768
ATTN_DIM = 8192


def setup_inputs(seed: int = 0, part: int = 0) -> dict:
    part_key = jax.random.fold_in(jax.random.key(seed), part)
    key_ctx, key_act = jax.random.split(part_key)
    key_wo, key_wd = jax.random.split(jax.random.key(seed + 1))
    w_scale = (FFN_DIM + ATTN_DIM) ** -0.5
    attn_ctx = jax.random.normal(key_ctx, (TOKENS, ATTN_DIM), jnp.float32)
    mlp_act = jax.random.normal(key_act, (TOKENS, FFN_DIM), jnp.float32)
    w_attn_out = jax.random.normal(key_wo, (ATTN_DIM, HIDDEN), jnp.float32) * w_scale
    w_mlp_down = jax.random.normal(key_wd, (FFN_DIM, HIDDEN), jnp.float32) * w_scale
    return {
        "attn_ctx": attn_ctx.astype(jnp.bfloat16),
        "w_attn_out": w_attn_out.astype(jnp.bfloat16),
        "mlp_act": mlp_act.astype(jnp.bfloat16),
        "w_mlp_down": w_mlp_down.astype(jnp.bfloat16),
    }


def reference(attn_ctx, w_attn_out, mlp_act, w_mlp_down):
    total = jnp.dot(attn_ctx, w_attn_out, preferred_element_type=jnp.float32)
    total = total + jnp.dot(mlp_act, w_mlp_down, preferred_element_type=jnp.float32)
    return total.astype(jnp.bfloat16)
```

```python
import jax
import jax.numpy as jnp
from jax import lax
from jax.experimental import pallas as pl
from jax.experimental.pallas import tpu as pltpu
from jax.sharding import PartitionSpec as P

MESH = pl.DeviceIdType.MESH
COLS = 256
DEPTH = 2048
SLOTS = 4


def _kernel(
    ctx, w_out, act, w_down, y,
    x, w, acc, part, sib_part, chip, far_chip, done,
    x_sem, w_sem, sib_send, sib_recv, far_send, far_recv, y_sem, y_send, y_recv,
    sib_free, far_free,
):
    rows = y.shape[0]
    half = rows // 2
    tiles = y.shape[1] // COLS
    ctx_depth = ctx.shape[1]
    chunks = x.shape[1] // DEPTH
    ctx_chunks = ctx_depth // DEPTH

    me = lax.axis_index("tp")
    core = lax.rem(me, 2)
    sib = {"tp": me + 1 - 2 * core}
    far = {"tp": lax.rem(me + 2, 4)}
    own_row = pl.multiple_of(core * half, half)
    sib_row = pl.multiple_of((1 - core) * half, half)

    def columns(j):
        return pl.ds(pl.multiple_of(j * COLS, COLS), COLS)

    def load_x(part_i, i):
        row = sib_row if part_i == 0 else own_row
        if i < ctx_chunks:
            src = ctx.at[pl.ds(row, half), pl.ds(i * DEPTH, DEPTH)]
        else:
            src = act.at[pl.ds(row, half), pl.ds((i - ctx_chunks) * DEPTH, DEPTH)]
        dst = x.at[pl.ds(part_i * half, half), pl.ds(i * DEPTH, DEPTH)]
        return pltpu.make_async_copy(src, dst, x_sem.at[part_i, i])

    def load_w(j, i):
        s = lax.rem(j, 2)
        if i < ctx_chunks:
            src = w_out.at[pl.ds(i * DEPTH, DEPTH), columns(j)]
        else:
            src = w_down.at[pl.ds((i - ctx_chunks) * DEPTH, DEPTH), columns(j)]
        return pltpu.make_async_copy(src, w.at[s, pl.ds(i * DEPTH, DEPTH), :], w_sem.at[s, i])

    def send_part(j):
        s = lax.rem(j, 2)
        return pltpu.make_async_remote_copy(
            part.at[s], sib_part.at[s], sib_send.at[s], sib_recv.at[s],
            device_id=sib, device_id_type=MESH)

    def send_chip(j):
        s = lax.rem(j, SLOTS)
        return pltpu.make_async_remote_copy(
            chip.at[s], far_chip.at[s], far_send.at[s], far_recv.at[s],
            device_id=far, device_id_type=MESH)

    def store_y(j):
        s = lax.rem(j, 2)
        return pltpu.make_async_copy(done.at[s], y.at[pl.ds(own_row, half), columns(j)], y_sem.at[s])

    def send_y(j):
        s = lax.rem(j, 2)
        return pltpu.make_async_remote_copy(
            done.at[s], y.at[pl.ds(own_row, half), columns(j)],
            y_send.at[s], y_recv.at[lax.rem(j, SLOTS)],
            device_id=sib, device_id_type=MESH)

    def chip_sum(j):
        total = acc[...] + sib_part[lax.rem(j, 2)].astype(jnp.float32)
        chip[lax.rem(j, SLOTS)] = total.astype(jnp.bfloat16)

    def final_sum(j):
        s = lax.rem(j, SLOTS)
        total = chip[s].astype(jnp.float32) + far_chip[s].astype(jnp.float32)
        done[lax.rem(j, 2)] = total.astype(jnp.bfloat16)

    for i in range(chunks):
        load_w(0, i).start()
        load_x(0, i).start()
    for i in range(chunks):
        load_x(1, i).start()
    for i in range(chunks):
        load_w(1, i).start()

    barrier = pltpu.get_barrier_semaphore()
    for peer in (sib, far):
        pl.semaphore_signal(barrier, inc=1, device_id=peer, device_id_type=MESH)
    pl.semaphore_wait(barrier, 2)

    for part_i in range(2):
        for i in range(chunks):
            if part_i == 0:
                load_w(0, i).wait()
            load_x(part_i, i).wait()
            depth = pl.ds(i * DEPTH, DEPTH)
            term = jnp.dot(x[pl.ds(part_i * half, half), depth], w[0, depth, :],
                           preferred_element_type=jnp.float32)
            if i == 0:
                acc[...] = term
            else:
                acc[...] += term
        if part_i == 0:
            part[0] = acc[...].astype(jnp.bfloat16)
            send_part(0).start()

    def wait_chip_inputs(j):
        send_part(j).wait_recv()

        @pl.when(j >= SLOTS)
        def _():
            send_chip(j - SLOTS).wait_send()
            pl.semaphore_wait(far_free, 1)

    def wait_final_inputs(j):
        send_chip(j).wait_recv()

        @pl.when(j >= 2)
        def _():
            store_y(j - 2).wait()
            send_y(j - 2).wait_send()
            send_y(j - 2).wait_recv()

    def finish_chip(j):
        chip_sum(j)
        send_chip(j).start()

    def finish_final(j):
        final_sum(j)
        store_y(j).start()
        send_y(j).start()

    def free_sib(j):
        @pl.when(j + 2 < tiles)
        def _():
            pl.semaphore_signal(sib_free, inc=1, device_id=sib, device_id_type=MESH)

    def free_far(j):
        @pl.when(j + SLOTS < tiles)
        def _():
            pl.semaphore_signal(far_free, inc=1, device_id=far, device_id_type=MESH)

    def tile(j, with_final):
        for i in range(chunks):
            load_w(j, i).wait()
        wait_chip_inputs(j - 1)
        if with_final:
            wait_final_inputs(j - 3)

        @pl.when(j >= 2)
        def _():
            send_part(j - 2).wait_send()
            pl.semaphore_wait(sib_free, 1)

        @pl.when(j + 1 < tiles)
        def _():
            for i in range(chunks):
                load_w(j + 1, i).start()

        s = lax.rem(j, 2)

        def one_half(h, carry):
            @pl.when(h == 0)
            def _():
                finish_chip(j - 1)

            if with_final:
                @pl.when(h == 1)
                def _():
                    finish_final(j - 3)

            row = pl.multiple_of(h * half, half)
            acc[...] = jnp.dot(x[pl.ds(row, half), :], w[s], preferred_element_type=jnp.float32)

            @pl.when(h == 0)
            def _():
                part[s] = acc[...].astype(jnp.bfloat16)
                send_part(j).start()

            return carry

        lax.fori_loop(0, 2, one_half, 0)
        free_sib(j - 1)
        if with_final:
            free_far(j - 3)

    def early(j, carry):
        tile(j, False)
        return carry

    def steady(j, carry):
        tile(j, True)
        return carry

    lax.fori_loop(1, 3, early, 0)
    lax.fori_loop(3, tiles, steady, 0)

    last = tiles - 1
    wait_chip_inputs(last)
    finish_chip(last)
    for j in range(tiles - 3, tiles):
        wait_final_inputs(j)
        finish_final(j)
    for j in range(tiles - 2, tiles):
        store_y(j).wait()
        send_y(j).wait_send()
        send_y(j).wait_recv()
        send_part(j).wait_send()
    for j in range(tiles - SLOTS, tiles):
        send_chip(j).wait_send()


def solution(mesh):
    def device_step(ctx, w_out, act, w_down):
        rows, depth = ctx.shape[0], ctx.shape[1] + act.shape[1]
        half, width = rows // 2, w_out.shape[1]
        piece = (half, COLS)
        sem = pltpu.SemaphoreType.DMA
        return pl.pallas_call(
            _kernel,
            out_shape=jax.ShapeDtypeStruct((rows, width), jnp.bfloat16),
            in_specs=[pl.BlockSpec(memory_space=pl.ANY)] * 4,
            out_specs=pl.BlockSpec(memory_space=pl.ANY),
            scratch_shapes=[
                pltpu.VMEM((rows, depth), jnp.bfloat16),
                pltpu.VMEM((2, depth, COLS), jnp.bfloat16),
                pltpu.VMEM(piece, jnp.float32),
                pltpu.VMEM((2, *piece), jnp.bfloat16),
                pltpu.VMEM((2, *piece), jnp.bfloat16),
                pltpu.VMEM((SLOTS, *piece), jnp.bfloat16),
                pltpu.VMEM((SLOTS, *piece), jnp.bfloat16),
                pltpu.VMEM((2, *piece), jnp.bfloat16),
                sem((2, depth // DEPTH)),
                sem((2, depth // DEPTH)),
                sem((2,)), sem((2,)),
                sem((SLOTS,)), sem((SLOTS,)),
                sem((2,)), sem((2,)), sem((SLOTS,)),
                pltpu.SemaphoreType.REGULAR,
                pltpu.SemaphoreType.REGULAR,
            ],
            compiler_params=pltpu.CompilerParams(
                collective_id=0, has_side_effects=True, vmem_limit_bytes=67043328),
            cost_estimate=pl.CostEstimate(
                flops=2 * rows * depth * width, transcendentals=0,
                bytes_accessed=2 * (rows * depth + depth * width + rows * width)),
        )(ctx, w_out, act, w_down)

    return jax.shard_map(
        device_step,
        mesh=mesh,
        in_specs=(P("data", "tp"), P("tp", None), P("data", "tp"), P("tp", None)),
        out_specs=P("data", None),
        check_vma=False,
    )
```

```python
import jax
import jax.numpy as jnp
from jax import lax
from jax.experimental import pallas as pl
from jax.experimental.pallas import tpu as pltpu
from jax.sharding import PartitionSpec as P

MESH = pl.DeviceIdType.MESH
COLS = 256
DEPTH = 2048
LAG = 5
SLOTS = 2 * LAG - 1


def _kernel(
    ctx, w_out, act, w_down, y,
    x, w, sib_acc, acc, part, sib_part, chip, far_chip, done,
    x_sem, w_sem, sib_send, sib_recv, far_send, far_recv, y_sem, y_send, y_recv,
):
    rows = y.shape[0]
    half = rows // 2
    piece = half // 2
    tiles = y.shape[1] // COLS
    phases = 2 * tiles
    chunks = x.shape[1] // DEPTH
    ctx_depth = ctx.shape[1]
    ctx_chunks = ctx_depth // DEPTH

    me = lax.axis_index("tp")
    core = lax.rem(me, 2)
    sib = {"tp": me + 1 - 2 * core}
    far = {"tp": lax.rem(me + 2, 4)}
    own_row = pl.multiple_of(core * half, half)
    sib_row = pl.multiple_of((1 - core) * half, half)

    def columns(p):
        return pl.ds(pl.multiple_of(lax.rem(p, tiles) * COLS, COLS), COLS)

    def load_x(h, side, i):
        row = pl.multiple_of((sib_row if side == 0 else own_row) + h * piece, piece)
        if i < ctx_chunks:
            src = ctx.at[pl.ds(row, piece), pl.ds(i * DEPTH, DEPTH)]
        else:
            src = act.at[pl.ds(row, piece), pl.ds((i - ctx_chunks) * DEPTH, DEPTH)]
        dst = x.at[pl.ds(side * piece, piece), pl.ds(i * DEPTH, DEPTH)]
        return pltpu.make_async_copy(src, dst, x_sem.at[side, i])

    def load_w(p):
        s = lax.rem(p, 2)
        return (
            pltpu.make_async_copy(
                w_out.at[:, columns(p)], w.at[s, pl.ds(0, ctx_depth), :], w_sem.at[s, 0]),
            pltpu.make_async_copy(
                w_down.at[:, columns(p)], w.at[s, pl.ds(ctx_depth, w_down.shape[0]), :],
                w_sem.at[s, 1]),
        )

    def send_part(p):
        return pltpu.make_async_remote_copy(
            part.at[lax.rem(p, 2)], sib_part.at[lax.rem(p, 4)],
            sib_send.at[lax.rem(p, 2)], sib_recv.at[lax.rem(p, 4)],
            device_id=sib, device_id_type=MESH)

    def send_chip(p):
        s = lax.rem(p, SLOTS)
        return pltpu.make_async_remote_copy(
            chip.at[s], far_chip.at[s], far_send.at[s], far_recv.at[s],
            device_id=far, device_id_type=MESH)

    def y_block(p):
        row = pl.multiple_of(own_row + p // tiles * piece, piece)
        return y.at[pl.ds(row, piece), columns(p)]

    def store_y(p):
        s = lax.rem(p, 2)
        return pltpu.make_async_copy(done.at[s], y_block(p), y_sem.at[s])

    def send_y(p):
        s = lax.rem(p, 2)
        return pltpu.make_async_remote_copy(
            done.at[s], y_block(p), y_send.at[s], y_recv.at[lax.rem(p, 4)],
            device_id=sib, device_id_type=MESH)

    def chip_sum(p):
        total = acc[lax.rem(p, 2)] + sib_part[lax.rem(p, 4)].astype(jnp.float32)
        chip[lax.rem(p, SLOTS)] = total.astype(jnp.bfloat16)

    def final_sum(p):
        s = lax.rem(p, SLOTS)
        total = chip[s].astype(jnp.float32) + far_chip[s].astype(jnp.float32)
        done[lax.rem(p, 2)] = total.astype(jnp.bfloat16)

    def finish_chip(p):
        send_part(p).wait_recv()

        @pl.when(p >= SLOTS)
        def _():
            send_chip(p - SLOTS).wait_send()

        chip_sum(p)
        send_chip(p).start()

    def wait_final(p):
        send_chip(p).wait_recv()

        @pl.when(p >= 2)
        def _():
            store_y(p - 2).wait()
            send_y(p - 2).wait_send()
            send_y(p - 2).wait_recv()

    def start_y(p):
        store_y(p).start()
        send_y(p).start()

    def dot(side, depth, slot):
        return jnp.dot(x[pl.ds(side * piece, piece), depth], w[slot, depth, :],
                       preferred_element_type=jnp.float32)

    first_w = load_w(0)
    first_w[0].start()
    for i in range(chunks):
        for side in range(2):
            load_x(0, side, i).start()
        if i == 0:
            first_w[1].start()

    barrier = pltpu.get_barrier_semaphore()
    for peer in (sib, far):
        pl.semaphore_signal(barrier, inc=1, device_id=peer, device_id_type=MESH)
    pl.semaphore_wait(barrier, 2)

    def prepare(p, with_final):
        @pl.when(p >= 2)
        def _():
            finish_chip(p - 2)
            send_part(p - 2).wait_send()

        if with_final:
            wait_final(p - LAG)

        @pl.when(p + 1 < phases)
        def _():
            for copy in load_w(p + 1):
                copy.start()

    def whole(p, with_final):
        for copy in load_w(p):
            copy.wait()
        prepare(p, with_final)
        s = lax.rem(p, 2)
        if with_final:
            final_sum(p - LAG)
        everything = pl.ds(0, x.shape[1])
        part[s] = dot(0, everything, s).astype(jnp.bfloat16)
        acc[s] = dot(1, everything, s)
        send_part(p).start()
        if with_final:
            start_y(p - LAG)

    def chunked(p, arrives, leaves, with_final):
        copies = load_w(p)
        copies[0].wait()
        if p > 0:
            copies[1].wait()
        prepare(p, with_final)
        s = p % 2
        for i in range(chunks):
            if arrives:
                for side in range(2):
                    load_x(p // tiles, side, i).wait()
            if p == 0 and i == 1:
                copies[1].wait()
            depth = pl.ds(i * DEPTH, DEPTH)
            sib_term, own_term = dot(0, depth, s), dot(1, depth, s)
            if i == 0:
                sib_acc[...] = sib_term
                acc[s] = own_term
            else:
                sib_acc[...] += sib_term
                acc[s] += own_term
            if leaves:
                for side in range(2):
                    load_x(p // tiles + 1, side, i).start()
        part[s] = sib_acc[...].astype(jnp.bfloat16)
        send_part(p).start()
        if with_final:
            final_sum(p - LAG)
            start_y(p - LAG)

    def early(p, carry):
        whole(p, False)
        return carry

    def steady(p, carry):
        whole(p, True)
        return carry

    chunked(0, True, False, False)
    lax.fori_loop(1, LAG, early, 0)
    lax.fori_loop(LAG, tiles - 1, steady, 0)
    chunked(tiles - 1, False, True, True)
    chunked(tiles, True, False, True)
    lax.fori_loop(tiles + 1, phases, steady, 0)

    for p in range(phases - 2, phases):
        finish_chip(p)
    for p in range(phases - LAG, phases):
        wait_final(p)
        final_sum(p)
        start_y(p)
    for p in range(phases - 2, phases):
        store_y(p).wait()
        send_y(p).wait_send()
        send_y(p).wait_recv()
        send_part(p).wait_send()
    for p in range(phases - SLOTS, phases):
        send_chip(p).wait_send()


def solution(mesh):
    def device_step(ctx, w_out, act, w_down):
        rows, depth = ctx.shape[0], ctx.shape[1] + act.shape[1]
        width = w_out.shape[1]
        piece = (rows // 4, COLS)
        sem = pltpu.SemaphoreType.DMA
        bf16, f32 = jnp.bfloat16, jnp.float32
        return pl.pallas_call(
            _kernel,
            out_shape=jax.ShapeDtypeStruct((rows, width), bf16),
            in_specs=[pl.BlockSpec(memory_space=pl.ANY)] * 4,
            out_specs=pl.BlockSpec(memory_space=pl.ANY),
            scratch_shapes=[
                pltpu.VMEM((rows // 2, depth), bf16),
                pltpu.VMEM((2, depth, COLS), bf16),
                pltpu.VMEM(piece, f32),
                pltpu.VMEM((2, *piece), f32),
                pltpu.VMEM((2, *piece), bf16),
                pltpu.VMEM((4, *piece), bf16),
                pltpu.VMEM((SLOTS, *piece), bf16),
                pltpu.VMEM((SLOTS, *piece), bf16),
                pltpu.VMEM((2, *piece), bf16),
                sem((2, depth // DEPTH)), sem((2, 2)),
                sem((2,)), sem((4,)),
                sem((SLOTS,)), sem((SLOTS,)),
                sem((2,)), sem((2,)), sem((4,)),
            ],
            compiler_params=pltpu.CompilerParams(
                collective_id=0, has_side_effects=True, vmem_limit_bytes=67043328),
            cost_estimate=pl.CostEstimate(
                flops=2 * rows * depth * width, transcendentals=0,
                bytes_accessed=2 * (rows * depth + depth * width + rows * width)),
        )(ctx, w_out, act, w_down)

    return jax.shard_map(
        device_step,
        mesh=mesh,
        in_specs=(P("data", "tp"), P("tp", None), P("data", "tp"), P("tp", None)),
        out_specs=P("data", None),
        check_vma=False,
    )
```
